32 devices in a mesh: grp: 2 (over y), shot: 4 (over x, core), slab: 4 (over z).
Axes of the slice: x: 2, y: 2, z: 4, core: 2. Of those that a mesh axis runs over, the one named last changes fastest.
Arguments:
- courant_sq: float32 [512, 1024], P(('grp', 'slab')), parts along dimension 0, may hold values from 0.05 to 0.25
- sponge_level: int32 [512, 1024], P(('grp', 'slab')), parts along dimension 0, may hold values from 0 to 3
- source_later: float32 [16, 256, 1024], P(('grp', 'shot'), 'slab'), parts along dimension 0, may hold values from -6 to 6
- source_now: float32 [16, 256, 1024], P(('grp', 'shot'), 'slab'), parts along dimension 0, may hold values from -6 to 6
- receiver_later: float32 [16, 256, 1024], P(('grp', 'shot'), 'slab'), parts along dimension 0, may hold values from -6 to 6
- receiver_now: float32 [16, 256, 1024], P(('grp', 'shot'), 'slab'), parts along dimension 0, may hold values from -6 to 6
- traces: float32 [16, 16, 512], P(('grp', 'shot')), parts along dimension 0, may hold values from -24 to 24
- wavelet: float32 [512], P('grp'), parts along dimension 0, may hold values from -24 to 24
- source_depth: int32 [16], P(('grp', 'shot')), parts along dimension 0, may hold values from 0 to 255
- source_lateral: int32 [16], P(('grp', 'shot')), parts along dimension 0, may hold values from 0 to 1023
- receiver_depth: int32 [16, 512], P(('grp', 'shot')), parts along dimension 0, may hold values from 0 to 255
- receiver_lateral: int32 [16, 512], P(('grp', 'shot')), parts along dimension 0, may hold values from 0 to 1023
- checkpoint_step: int32 [16], P(('grp', 'shot')), parts along dimension 0, may hold values from 0 to 240
Outputs:
- image: float32 [512, 1024], P(('grp', 'slab')), parts along dimension 0
- source_out: float32 [16, 256, 1024], P(('grp', 'shot'), 'slab'), parts along dimension 0
- receiver_out: float32 [16, 256, 1024], P(('grp', 'shot'), 'slab'), parts along dimension 0
The draws below stay inside these ranges and needn't reach their ends.
There are 2 independent parts, one for each index of `grp`. The reference program is written for one: setup_inputs(seed, part) draws one part's arguments, and reference() takes and returns one part's arrays. A program takes and returns all parts, laid end to end along the dimension named above; each array names one. Nothing has to cross between parts.
All inputs are finite; a program needn't handle non-finite values.
Results may differ from the reference program's by a relative error of at most 0.0003.
Values sent between devices are 32-bit elements; how exact they have to be, the bound alone decides.
A program may use at most 64 MiB of HBM per device.

```python
import math
import jax
import jax.numpy as jnp
from jax import lax

NX = 1024
STEPS = 16
NREC = 512
NT = 256
NZ = 256
SHOTS = 8


def with_ends(drawn, stream_key, smallest, largest):
    dims = drawn.shape
    place = [jax.random.randint(jax.random.fold_in(stream_key, axis), (), 0, dims[axis]) for axis in range(len(dims))]
    drawn = drawn.at[tuple(place)].set(smallest)
    longest = dims.index(max(dims))
    place[longest] = (place[longest] + 1) % dims[longest]
    return drawn.at[tuple(place)].set(largest)


def level_of(key, shape, split, least, top_value):
    factor_of, own = 1.0, jax.random.fold_in(key, 6)
    for position, shards_of in split:
        steps = jnp.exp(jax.random.uniform(jax.random.fold_in(own, position), (shards_of,), jnp.float32, least / len(split), top_value / len(split)))
        factor_of = factor_of * jnp.repeat(steps, shape[position] // shards_of).reshape([-1 if axis == position else 1 for axis in range(len(shape))])
    return factor_of


def normal_values(key, dims, spread, most, split=(), kind=jnp.bfloat16):
    values = spread * jax.random.normal(key, dims, jnp.float32)
    if split:
        values = values * level_of(key, dims, split, -0.22, 0.18)
    return jnp.clip(values, -most, most).astype(kind)


def setup_inputs(seed: int = 0, part: int = 0) -> dict:
    streams_of = jax.random.split(jax.random.key(seed), 14)
    own_keys = jax.random.split(jax.random.fold_in(streams_of[13], part), 14)
    return {
        "courant_sq": jnp.clip(jnp.exp(math.log(0.25) - 1.609438 * jax.random.uniform(own_keys[0], (NZ, NX), jnp.float32) ** level_of(own_keys[0], (NZ, NX), ((0, 4),), -0.2, 0.2)), 0.05, 0.25),
        "sponge_level": with_ends(jax.random.randint(own_keys[1], (NZ, NX), 0, 4), jax.random.fold_in(own_keys[1], 1), 0, 3).astype(jnp.int32),
        "source_later": normal_values(own_keys[2], (SHOTS, NZ, NX), 1.0, 6.0, ((0, 4), (1, 4)), jnp.float32),
        "source_now": normal_values(own_keys[3], (SHOTS, NZ, NX), 1.0, 6.0, ((0, 4), (1, 4)), jnp.float32),
        "receiver_later": normal_values(own_keys[4], (SHOTS, NZ, NX), 1.0, 6.0, ((0, 4), (1, 4)), jnp.float32),
        "receiver_now": normal_values(own_keys[5], (SHOTS, NZ, NX), 1.0, 6.0, ((0, 4), (1, 4)), jnp.float32),
        "traces": normal_values(own_keys[6], (SHOTS, STEPS, NREC), 4.0, 24.0, ((0, 4),), jnp.float32),
        "wavelet": normal_values(own_keys[7], (NT,), 4.0, 24.0, (), jnp.float32),
        "source_depth": with_ends(jax.random.randint(own_keys[8], (SHOTS,), 0, NZ), jax.random.fold_in(own_keys[8], 1), 0, NZ - 1).astype(jnp.int32),
        "source_lateral": with_ends(jax.random.randint(own_keys[9], (SHOTS,), 0, NX), jax.random.fold_in(own_keys[9], 1), 0, NX - 1).astype(jnp.int32),
        "receiver_depth": with_ends(jax.random.randint(own_keys[10], (SHOTS, NREC), 0, NZ), jax.random.fold_in(own_keys[10], 1), 0, NZ - 1).astype(jnp.int32),
        "receiver_lateral": with_ends(jax.random.randint(own_keys[11], (SHOTS, NREC), 0, NX), jax.random.fold_in(own_keys[11], 1), 0, NX - 1).astype(jnp.int32),
        "checkpoint_step": with_ends(jax.random.randint(own_keys[12], (SHOTS,), 0, NT - STEPS + 1), jax.random.fold_in(own_keys[12], 1), 0, NT - STEPS).astype(jnp.int32),
    }


stencil_coeffs = (-205.0 / 72.0, 8.0 / 5.0, -1.0 / 5.0, 8.0 / 315.0, -1.0 / 560.0)

def laplace(extended):
    row_count = extended.shape[-2] - 8
    width = extended.shape[-1]
    centre = extended[..., 4:4 + row_count, :]
    pad_spec = [(0, 0)] * (centre.ndim - 1) + [(4, 4)]
    padded = jnp.pad(centre, pad_spec)
    result = 2.0 * stencil_coeffs[0] * centre
    for offset in range(1, 5):
        result = result + stencil_coeffs[offset] * (extended[..., 4 + offset:4 + offset + row_count, :] + extended[..., 4 - offset:4 - offset + row_count, :] + padded[..., 4 + offset:4 + offset + width] + padded[..., 4 - offset:4 - offset + width])
    return result

def reference(courant_sq, sponge_level, source_later, source_now, receiver_later, receiver_now, traces, wavelet, source_depth, source_lateral, receiver_depth, receiver_lateral, checkpoint_step):
    damping = 1.0 - 0.06 * sponge_level.astype(jnp.float32)

    def one_shot(image_sum, items):
        src_hi, src_now, rec_hi, rec_now, shot_traces, depth_src, lateral_src, depth_rec, lateral_rec, start = items
        for step_index in range(STEPS):
            image_sum = image_sum + src_now * rec_now
            both = jnp.pad(jnp.stack([src_now, rec_now]), ((0, 0), (4, 4), (0, 0)))
            laplacian = laplace(both)
            pulse = wavelet[start + STEPS - 1 - step_index]
            src_next = 2.0 * src_now - src_hi + courant_sq * laplacian[0]
            src_next = src_next.at[depth_src, lateral_src].add(-(courant_sq[depth_src, lateral_src] * pulse))
            rec_next = 2.0 * rec_now - rec_hi + courant_sq * laplacian[1]
            rec_next = rec_next.at[depth_rec, lateral_rec].add(courant_sq[depth_rec, lateral_rec] * shot_traces[step_index])
            rec_next = damping * rec_next
            src_hi, src_now, rec_hi, rec_now = (src_now, src_next, rec_now, rec_next)
        return (image_sum, (src_now, rec_now))
    start_image = jnp.zeros(courant_sq.shape, jnp.float32)
    image_sum, (source_out, receiver_out) = lax.scan(one_shot, start_image, (source_later, source_now, receiver_later, receiver_now, traces, source_depth, source_lateral, receiver_depth, receiver_lateral, checkpoint_step))
    image = image_sum / math.sqrt(STEPS * SHOTS)
    return (image, source_out, receiver_out)
```

```python
import functools
import math

import jax
import jax.numpy as jnp
from jax import lax
from jax.experimental import pallas as pl
from jax.experimental.pallas import tpu as pltpu
from jax.sharding import PartitionSpec as P

STEPS = 16
PAIRS = STEPS // 2
MESH = pl.DeviceIdType.MESH
LANES = 128
HALO = 8

coeffs = (-205.0 / 72.0, 8.0 / 5.0, -1.0 / 5.0, 8.0 / 315.0, -1.0 / 560.0)


def kernel(
    slabs,
    shot_devices,
    scale,
    wavelet,
    checkpoint,
    s_depth,
    s_lateral,
    velocity_in,
    sponge_in,
    s_later,
    s_now,
    r_later,
    r_now,
    traces,
    r_depth,
    table,
    image_out,
    s_out,
    r_out,
    even,
    odd,
    velocity,
    damping,
    source,
    corr,
    inject_1,
    inject_2,
    slots,
    start_fields,
    start_velocity,
    start_sponge,
    pair_buf,
    chip_src,
    chip_buf,
    last_src,
    last_buf,
    send_sem,
    recv_sem,
    start_send,
    start_recv,
    sum_send,
    sum_recv,
):
    shots, rows, width = s_now.shape
    blocks = width // LANES
    me = lax.axis_index("slab")
    shot_me = lax.axis_index("shot")
    has_up = me > 0
    has_down = me < slabs - 1
    up = jnp.maximum(me - 1, 0)
    down = jnp.minimum(me + 1, slabs - 1)
    first_row = me * rows
    lane = lax.broadcasted_iota(jnp.int32, (8, LANES), 1)
    sub = lax.broadcasted_iota(jnp.int32, (8, LANES), 0)
    zero = jnp.zeros((8, LANES), jnp.float32)

    barrier = pltpu.get_barrier_semaphore()

    @pl.when(has_up)
    def _():
        pl.semaphore_signal(barrier, inc=1, device_id={"slab": up}, device_id_type=MESH)

    @pl.when(has_down)
    def _():
        pl.semaphore_signal(barrier, inc=1, device_id={"slab": down}, device_id_type=MESH)

    for other in range(1, shot_devices):
        target = lax.rem(shot_me + other, shot_devices)
        pl.semaphore_signal(barrier, inc=1, device_id={"shot": target}, device_id_type=MESH)
    pl.semaphore_wait(
        barrier, shot_devices - 1 + has_up.astype(jnp.int32) + has_down.astype(jnp.int32)
    )

    def start_copies(side):
        first = 0 if side == 1 else rows - HALO
        target = up if side == 1 else down
        copies = []
        sources = [
            (s_now.at[:, pl.ds(first, HALO), :], start_fields.at[side, 0]),
            (s_later.at[:, pl.ds(first, HALO), :], start_fields.at[side, 1]),
            (velocity_in.at[pl.ds(first, HALO), :], start_velocity.at[side]),
            (r_now.at[:, pl.ds(first, HALO), :], start_fields.at[side, 2]),
            (r_later.at[:, pl.ds(first, HALO), :], start_fields.at[side, 3]),
            (sponge_in.at[pl.ds(first, HALO), :], start_sponge.at[side]),
        ]
        for number, (src, dst) in enumerate(sources):
            copies.append(
                pltpu.make_async_remote_copy(
                    src_ref=src,
                    dst_ref=dst,
                    send_sem=start_send.at[side, number],
                    recv_sem=start_recv.at[side, number],
                    device_id={"slab": target},
                    device_id_type=MESH,
                )
            )
        return copies

    @pl.when(has_up)
    def _():
        for copy in start_copies(1):
            copy.start()

    @pl.when(has_down)
    def _():
        for copy in start_copies(0):
            copy.start()

    def put_rows(row, side_now, side_later, velocity_rows, sponge_rows):
        for j in range(blocks):
            cut = pl.ds(j * LANES, LANES)
            speed = velocity_rows(cut)
            velocity[j, pl.ds(row, 8), :] = speed
            damping[j, pl.ds(row, 8), :] = 1.0 - 0.06 * sponge_rows(cut).astype(jnp.float32)
            row_ids = first_row - HALO + row + sub
            column_ids = j * LANES + lane
            for s in range(shots):
                hit = (row_ids == s_depth[s]) & (column_ids == s_lateral[s])
                source[s, j, pl.ds(row, 8), :] = jnp.where(hit, -speed, 0.0)
                for f in range(2):
                    even[2 * s + f, j, pl.ds(row, 8), :] = side_now(f, s, cut)
                    odd[2 * s + f, j, pl.ds(row, 8), :] = side_later(f, s, cut)

    for tile in range(rows // 8):
        r = tile * 8
        put_rows(
            HALO + r,
            lambda f, s, cut: (s_now, r_now)[f][s, pl.ds(r, 8), cut],
            lambda f, s, cut: (s_later, r_later)[f][s, pl.ds(r, 8), cut],
            lambda cut: velocity_in[pl.ds(r, 8), cut],
            lambda cut: sponge_in[pl.ds(r, 8), cut],
        )
        for j in range(blocks):
            cut = pl.ds(j * LANES, LANES)
            total = s_now[0, pl.ds(r, 8), cut] * r_now[0, pl.ds(r, 8), cut]
            for s in range(1, shots):
                total = total + s_now[s, pl.ds(r, 8), cut] * r_now[s, pl.ds(r, 8), cut]
            corr[j, pl.ds(r, 8), :] = total

    for side, present, row in ((0, has_up, 0), (1, has_down, HALO + rows)):

        @pl.when(present)
        def _():
            for copy in start_copies(1 - side):
                copy.wait_send()
            for copy in start_copies(side):
                copy.wait_recv()
            put_rows(
                row,
                lambda f, s, cut: start_fields[side, 2 * f, s, :, cut],
                lambda f, s, cut: start_fields[side, 2 * f + 1, s, :, cut],
                lambda cut: start_velocity[side, :, cut],
                lambda cut: start_sponge[side, :, cut],
            )

        @pl.when(jnp.logical_not(present))
        def _():
            for j in range(blocks):
                velocity[j, pl.ds(row, 8), :] = zero
                damping[j, pl.ds(row, 8), :] = zero
                for s in range(shots):
                    source[s, j, pl.ds(row, 8), :] = zero
                    for f in range(2):
                        even[2 * s + f, j, pl.ds(row, 8), :] = zero
                        odd[2 * s + f, j, pl.ds(row, 8), :] = zero

    def laplace_rows(ref, w, row, j, centre):
        total = (2.0 * coeffs[0]) * centre[j]
        left = centre[j - 1] if j > 0 else zero
        right = centre[j + 1] if j < blocks - 1 else zero
        for k in range(1, 5):
            ahead = pltpu.roll(jnp.where(lane >= k, centre[j], right), LANES - k, 1)
            behind = pltpu.roll(jnp.where(lane < LANES - k, centre[j], left), k, 1)
            total = total + coeffs[k] * (
                (ref[w, j, pl.ds(row + k, 8), :] + ref[w, j, pl.ds(row - k, 8), :])
                + (ahead + behind)
            )
        return total

    def source_tile(now, later, s, row, pulse):
        w = 2 * s
        centre = [now[w, j, pl.ds(row, 8), :] for j in range(blocks)]
        for j in range(blocks):
            lap = laplace_rows(now, w, row, j, centre)
            later[w, j, pl.ds(row, 8), :] = (
                (centre[j] + centre[j] - later[w, j, pl.ds(row, 8), :])
                + velocity[j, pl.ds(row, 8), :] * lap
                + pulse * source[s, j, pl.ds(row, 8), :]
            )

    def receiver_tile(now, later, s, row, inject, inject_row):
        w = 2 * s + 1
        centre = [now[w, j, pl.ds(row, 8), :] for j in range(blocks)]
        for j in range(blocks):
            lap = laplace_rows(now, w, row, j, centre)
            lap = lap + inject[pl.ds(inject_row, 8), pl.ds(j * LANES, LANES)]
            later[w, j, pl.ds(row, 8), :] = damping[j, pl.ds(row, 8), :] * (
                (centre[j] + centre[j] - later[w, j, pl.ds(row, 8), :])
                + velocity[j, pl.ds(row, 8), :] * lap
            )

    def halo_copy(w, parity, side):
        first = HALO if side == 1 else rows
        target = up if side == 1 else down
        return pltpu.make_async_remote_copy(
            src_ref=even.at[w, :, pl.ds(first, HALO), :],
            dst_ref=slots.at[parity, side, w],
            send_sem=send_sem.at[parity, side, w],
            recv_sem=recv_sem.at[parity, side, w],
            device_id={"slab": target},
            device_id_type=MESH,
        )

    tiles = rows // 8

    def one_field(pair, s, f, step_1, step_2):
        w = 2 * s + f
        sent = lax.rem(pair + 1, 2)
        slot = lax.rem(pair, 2)
        for t in range(1, tiles):
            step_1(4 + 8 * t, 8 * t)
        for side, present, row in ((0, has_up, 0), (1, has_down, HALO + rows)):

            @pl.when(present & (pair > 0))
            def _():
                halo_copy(w, sent, 1 - side).wait_send()
                halo_copy(w, sent, side).wait_recv()
                for j in range(blocks):
                    even[w, j, pl.ds(row, 8), :] = slots[sent, side, w, j]

        step_1(4, 0)
        step_1(4 + rows, rows)
        step_2(HALO, 0)
        step_2(HALO + rows - 8, rows - 8)
        for side, present in ((1, has_up), (0, has_down)):

            @pl.when(present & (pair < PAIRS - 1))
            def _():
                halo_copy(w, slot, side).start()

        for t in range(1, tiles - 1):
            step_2(HALO + 8 * t, 8 * t)

    def injection(pair, s):
        ids = first_row + lax.broadcasted_iota(jnp.int32, (rows + 8, r_depth.shape[1]), 0)
        depth = r_depth[pl.ds(s, 1), :]
        hit_1 = (ids - 4) == depth
        hit_2 = ids[:rows] == depth
        parts = []
        for hit, step in ((hit_1, 2 * pair), (hit_2, 2 * pair + 1)):
            trace = traces[s, pl.ds(step, 1), :]
            high = trace.astype(jnp.bfloat16).astype(jnp.float32)
            parts.append(jnp.where(hit, high, 0.0))
            parts.append(jnp.where(hit, trace - high, 0.0))
        stacked = jnp.concatenate(parts, axis=0).astype(jnp.bfloat16)
        wide = 2 * LANES
        one = rows + 8
        for n in range(width // wide):
            cut = pl.ds(n * wide, wide)
            out = jnp.dot(stacked, table[s, :, cut], preferred_element_type=jnp.float32)
            inject_1[:, cut] = out[:one] + out[one : 2 * one]
            inject_2[:, cut] = out[2 * one : 2 * one + rows] + out[2 * one + rows :]

    def shot_pair(pair, s):
        step = checkpoint[s] + STEPS - 1 - 2 * pair
        pulse_1 = wavelet[step]
        pulse_2 = wavelet[step - 1]

        @pl.when(pair > 0)
        def _():
            for t in range(tiles):
                for j in range(blocks):
                    cut = pl.ds(HALO + 8 * t, 8)
                    corr[j, pl.ds(8 * t, 8), :] += even[2 * s, j, cut, :] * even[2 * s + 1, j, cut, :]

        one_field(
            pair,
            s,
            0,
            lambda row, _: source_tile(even, odd, s, row, pulse_1),
            lambda row, _: source_tile(odd, even, s, row, pulse_2),
        )
        injection(pair, s)
        one_field(
            pair,
            s,
            1,
            lambda row, at: receiver_tile(even, odd, s, row, inject_1, at),
            lambda row, at: receiver_tile(odd, even, s, row, inject_2, at),
        )
        for t in range(tiles):
            for j in range(blocks):
                cut = pl.ds(HALO + 8 * t, 8)
                corr[j, pl.ds(8 * t, 8), :] += odd[2 * s, j, cut, :] * odd[2 * s + 1, j, cut, :]

    def turn(index, carry):
        shot_pair(index // shots, lax.rem(index, shots))
        return carry

    lax.fori_loop(0, PAIRS * shots, turn, 0)

    half = rows // 2
    odd_one = lax.rem(shot_me, 2)
    mate = shot_me + 1 - 2 * odd_one
    keep = pl.multiple_of(odd_one * half, 8)
    give = pl.multiple_of((1 - odd_one) * half, 8)
    chips = shot_devices // 2
    first = pltpu.make_async_remote_copy(
        src_ref=corr.at[:, pl.ds(give, half), :],
        dst_ref=pair_buf,
        send_sem=sum_send.at[0],
        recv_sem=sum_recv.at[0],
        device_id={"shot": mate},
        device_id_type=MESH,
    )
    first.start()
    for t in range(rows // 8):
        for j in range(blocks):
            for s in range(shots):
                cut = pl.ds(HALO + 8 * t, 8)
                s_out[s, pl.ds(8 * t, 8), pl.ds(j * LANES, LANES)] = even[2 * s, j, cut, :]
                r_out[s, pl.ds(8 * t, 8), pl.ds(j * LANES, LANES)] = even[2 * s + 1, j, cut, :]
    first.wait()
    chip_src[...] = corr[:, pl.ds(keep, half), :] + pair_buf[...]
    others = []
    for other in range(1, chips):
        target = lax.rem(shot_me + 2 * other, shot_devices)
        copy = pltpu.make_async_remote_copy(
            src_ref=chip_src,
            dst_ref=chip_buf.at[other - 1],
            send_sem=sum_send.at[1 + other],
            recv_sem=sum_recv.at[1 + other],
            device_id={"shot": target},
            device_id_type=MESH,
        )
        copy.start()
        others.append(copy)
    total = chip_src[...]
    for number, copy in enumerate(others):
        copy.wait()
        total = total + chip_buf[number]
    last_src[...] = total * scale
    last = pltpu.make_async_remote_copy(
        src_ref=last_src,
        dst_ref=last_buf,
        send_sem=sum_send.at[1],
        recv_sem=sum_recv.at[1],
        device_id={"shot": mate},
        device_id_type=MESH,
    )
    last.start()
    for j in range(blocks):
        image_out[pl.ds(keep, half), pl.ds(j * LANES, LANES)] = last_src[j]
    last.wait()
    for j in range(blocks):
        image_out[pl.ds(give, half), pl.ds(j * LANES, LANES)] = last_buf[j]


def local(slabs, shot_devices, courant_sq, sponge_level, source_later, source_now, receiver_later,
          receiver_now, traces, wavelet, source_depth, source_lateral, receiver_depth,
          receiver_lateral, checkpoint_step):
    shots, rows, width = source_now.shape
    blocks = width // LANES
    wide = rows + 2 * HALO
    lateral_ids = jnp.arange(width, dtype=jnp.int32)
    table = (receiver_lateral[:, :, None] == lateral_ids[None, None, :]).astype(jnp.bfloat16)
    vmem = pl.BlockSpec(memory_space=pltpu.VMEM)
    smem = pl.BlockSpec(memory_space=pltpu.SMEM)
    f32 = jnp.float32
    half = rows // 2
    chips = shot_devices // 2
    return pl.pallas_call(
        functools.partial(kernel, slabs, shot_devices, 1.0 / math.sqrt(STEPS * shots * shot_devices)),
        out_shape=(
            jax.ShapeDtypeStruct((rows, width), f32),
            jax.ShapeDtypeStruct((shots, rows, width), f32),
            jax.ShapeDtypeStruct((shots, rows, width), f32),
        ),
        in_specs=[smem] * 4 + [vmem] * 9,
        out_specs=(vmem, vmem, vmem),
        scratch_shapes=[
            pltpu.VMEM((2 * shots, blocks, wide, LANES), f32),
            pltpu.VMEM((2 * shots, blocks, wide, LANES), f32),
            pltpu.VMEM((blocks, wide, LANES), f32),
            pltpu.VMEM((blocks, wide, LANES), f32),
            pltpu.VMEM((shots, blocks, wide, LANES), f32),
            pltpu.VMEM((blocks, rows, LANES), f32),
            pltpu.VMEM((rows + 8, width), f32),
            pltpu.VMEM((rows, width), f32),
            pltpu.VMEM((2, 2, 2 * shots, blocks, HALO, LANES), f32),
            pltpu.VMEM((2, 4, shots, HALO, width), f32),
            pltpu.VMEM((2, HALO, width), f32),
            pltpu.VMEM((2, HALO, width), jnp.int32),
            pltpu.VMEM((blocks, half, LANES), f32),
            pltpu.VMEM((blocks, half, LANES), f32),
            pltpu.VMEM((max(chips - 1, 1), blocks, half, LANES), f32),
            pltpu.VMEM((blocks, half, LANES), f32),
            pltpu.VMEM((blocks, half, LANES), f32),
            pltpu.SemaphoreType.DMA((2, 2, 2 * shots)),
            pltpu.SemaphoreType.DMA((2, 2, 2 * shots)),
            pltpu.SemaphoreType.DMA((2, 6)),
            pltpu.SemaphoreType.DMA((2, 6)),
            pltpu.SemaphoreType.DMA((chips + 1,)),
            pltpu.SemaphoreType.DMA((chips + 1,)),
        ],
        compiler_params=pltpu.CompilerParams(
            collective_id=0, has_side_effects=True, vmem_limit_bytes=48 * 1024 * 1024
        ),
        name="migrate",
    )(
        wavelet, checkpoint_step, source_depth, source_lateral, courant_sq, sponge_level,
        source_later, source_now, receiver_later, receiver_now, traces, receiver_depth, table,
    )


def solution(mesh):
    in_specs = (
        P(("grp", "slab"), None),
        P(("grp", "slab"), None),
        P(("grp", "shot"), "slab", None),
        P(("grp", "shot"), "slab", None),
        P(("grp", "shot"), "slab", None),
        P(("grp", "shot"), "slab", None),
        P(("grp", "shot"), None, None),
        P("grp"),
        P(("grp", "shot")),
        P(("grp", "shot")),
        P(("grp", "shot"), None),
        P(("grp", "shot"), None),
        P(("grp", "shot")),
    )
    out_specs = (
        P(("grp", "slab"), None),
        P(("grp", "shot"), "slab", None),
        P(("grp", "shot"), "slab", None),
    )
    return jax.shard_map(
        functools.partial(local, mesh.shape["slab"], mesh.shape["shot"]),
        mesh=mesh, in_specs=in_specs, out_specs=out_specs, check_vma=False,
    )
```
